32 devices in a mesh: tm: 8 (over y, x, core), space: 4 (over z).
Axes of the slice: x: 2, y: 2, z: 4, core: 2. Of those that a mesh axis runs over, the one named last changes fastest.
Arguments:
- initial_state: float32 [1024, 1024], P('space'), may hold values from -6 to 6
- guess_coarse: float32 [8, 1024, 1024], P('tm', 'space'), may hold values from -6 to 6
- force_fine: float32 [8, 1024, 1024], P('tm', 'space'), may hold values from -6 to 6
- force_coarse: float32 [8, 1024, 1024], P('tm', 'space'), may hold values from -6 to 6
- eigen_basis: float32 [1024, 1024], replicated, may hold values from -1 to 1, as said below
- eigen_rates: float32 [1024], replicated, may hold values from 0.02 to 4
- carried_correction: float32 [1024, 1024], replicated, may hold values from -6 to 6
Outputs:
- fine_states: float32 [8, 1024, 1024], P('tm', 'space')
- coarse_states: float32 [8, 1024, 1024], P('tm', 'space')
The draws below stay inside these ranges and needn't reach their ends.
Inputs may be any that keep to these rules, and one draw needn't show every extreme that they name: `eigen_basis`: an orthogonal matrix: its transpose is its inverse up to float32 rounding.
All inputs are finite; a program needn't handle non-finite values.
Results may differ from the reference program's by a relative error of at most 0.00013.
Values sent between devices are 32-bit elements; how exact they have to be, the bound alone decides.
No kernel may reach another device: no remote copies, remote signals or barrier semaphores. Data moves between devices by JAX's collectives and lax.ppermute only.
A program may use at most 128 MiB of HBM per device.

```python
import math
import jax
import jax.numpy as jnp
from jax import lax

GRID = 1024
GROUPS = 8


def draw_eigen_basis(key, part):
    skewed = jax.random.normal(key, (GRID, GRID), jnp.float32) / math.sqrt(GRID)
    skewed = skewed - skewed.T
    identity = jnp.eye(GRID, dtype=jnp.float32)
    return jnp.linalg.solve(identity + skewed, identity - skewed)


def shard_levels(stream_key, dims, split, least, high):
    level = 1.0
    for dim, shards_of in split:
        heights = jax.random.uniform(jax.random.fold_in(jax.random.fold_in(stream_key, 6), dim), (shards_of,), jnp.float32, least / len(split), high / len(split))
        level = level * jnp.repeat(jnp.exp(heights), dims[dim] // shards_of).reshape((-1,) + (1,) * (len(dims) - 1 - dim))
    return level


def scatter_about(key, shape, scale, most, pieces=(), kind=jnp.bfloat16):
    loudness = shard_levels(key, shape, pieces, -0.22, 0.18) if pieces else 1.0
    array = jax.random.normal(key, shape, jnp.float32) * scale * loudness
    return jnp.minimum(jnp.maximum(array, -most), most).astype(kind)


def setup_inputs(seed: int = 0) -> dict:
    key_of = jax.random.split(jax.random.key(seed), 8)
    return {
        "initial_state": scatter_about(key_of[0], (GRID, GRID), 1.0, 6.0, ((0, 4),), jnp.float32),
        "guess_coarse": scatter_about(key_of[1], (GROUPS, GRID, GRID), 1.0, 6.0, ((0, 8), (1, 4)), jnp.float32),
        "force_fine": scatter_about(key_of[2], (GROUPS, GRID, GRID), 1.0, 6.0, ((0, 8), (1, 4)), jnp.float32),
        "force_coarse": scatter_about(key_of[3], (GROUPS, GRID, GRID), 1.0, 6.0, ((0, 8), (1, 4)), jnp.float32),
        "eigen_basis": draw_eigen_basis(jax.random.fold_in(key_of[7], 71), 0),
        "eigen_rates": jnp.clip(jnp.exp(jax.random.uniform(key_of[5], (GRID,), jnp.float32, math.log(0.02), math.log(4.0))), 0.02, 4.0),
        "carried_correction": scatter_about(key_of[6], (GRID, GRID), 1.0, 6.0, (), jnp.float32),
    }


exact_mode = lax.Precision.HIGHEST

def reference(initial_state, guess_coarse, force_fine, force_coarse, eigen_basis, eigen_rates, carried_correction):
    fine_decay = 1.0 / (1.0 + eigen_rates[:, None] + eigen_rates[None, :])
    coarse_decay = 1.0 / (1.0 + 2.0 * (eigen_rates[:, None] + eigen_rates[None, :]))

    def to_eigen(field):
        right = jnp.einsum('gij,jk->gik', field, eigen_basis, precision=exact_mode)
        return jnp.einsum('ji,gjk->gik', eigen_basis, right, precision=exact_mode)

    def from_eigen(coeffs):
        left = jnp.einsum('ij,gjk->gik', eigen_basis, coeffs, precision=exact_mode)
        return jnp.einsum('gij,kj->gik', left, eigen_basis, precision=exact_mode)

    def reaction(field):
        return field + 0.5 * jnp.tanh(field)

    def propagate(field, source):
        return from_eigen(fine_decay[None] * to_eigen(reaction(field) + source))

    def previous(states):
        return jnp.concatenate([initial_state[None], states[:-1]], axis=0)
    relaxed_fine = propagate(previous(guess_coarse), force_fine)
    relaxed_coarse = propagate(relaxed_fine, force_coarse)
    second_fine = propagate(previous(relaxed_coarse), force_fine)
    residual = fine_decay[None] * to_eigen(reaction(second_fine) + force_coarse) - to_eigen(relaxed_coarse)

    def coarse_turn(carry, term):
        updated = coarse_decay * carry + term
        return (updated, updated)
    unused, correction = lax.scan(coarse_turn, carried_correction, residual)
    coarse_states = relaxed_coarse + from_eigen(correction)
    fine_states = propagate(previous(coarse_states), force_fine)
    return (fine_states, coarse_states)
```

```python
import jax
import jax.numpy as jnp
from jax import lax
from jax.sharding import PartitionSpec as P


both = ("tm", "space")


class Plan:
    def __init__(self, groups, blocks):
        self.groups, self.blocks, self.rounds = groups, blocks, blocks // 2
        self.low = blocks // 2 - 1

    def flat(self, t, s):
        return t * self.blocks + s

    def home(self, g, h):
        return self.flat(2 * (g // 2) + h, self.low + g % 2)

    def inward(self, r, shift):
        return [
            (self.flat(g, b), self.home(g - shift, b // self.rounds))
            for g in range(shift, self.groups)
            for b in range(self.blocks)
            if b % self.rounds == r
        ]

    def outward(self, r, shift, chains):
        return [
            (self.home(g, h), self.flat(g + shift, h * self.rounds + r))
            for g in chains
            for h in range(2)
        ]

    def partners(self):
        return [(t, t ^ 1) for t in range(self.groups)]

    def rings(self):
        used = [[self.home(g, h) for g in range(self.groups)] for h in range(2)]
        idle = [s for s in range(self.blocks) if s not in (self.low, self.low + 1)]
        return used + [[self.flat(t, s) for t in range(self.groups)] for s in idle]


def dot(left, right, dims=((1,), (0,))):
    return lax.dot_general(
        left,
        right,
        (dims, ((), ())),
        precision=lax.Precision.HIGH,
        preferred_element_type=jnp.float32,
    )


def reaction(field):
    return field + 0.5 * jnp.tanh(field)


def on_device(
    initial_state,
    guess_coarse,
    force_fine,
    force_coarse,
    eigen_basis,
    eigen_rates,
    carried_correction,
):
    groups, blocks = lax.axis_size("tm"), lax.axis_size("space")
    plan = Plan(groups, blocks)
    t, s = lax.axis_index("tm"), lax.axis_index("space")
    grid = eigen_basis.shape[0]
    half = grid // 2
    part = grid // groups
    block = initial_state.shape[0]
    h = t % 2
    chain = 2 * (t // 2) + jnp.clip(s - plan.low, 0, 1)
    mine, other = h * half, (1 - h) * half

    rows_mine = lax.dynamic_slice_in_dim(eigen_basis, mine, half, 0)
    rows_other = lax.dynamic_slice_in_dim(eigen_basis, other, half, 0)
    cols_mine = lax.dynamic_slice_in_dim(eigen_basis, mine, half, 1)
    cols_other = lax.dynamic_slice_in_dim(eigen_basis, other, half, 1)
    rates_mine = lax.dynamic_slice_in_dim(eigen_rates, mine, half, 0)
    sums = eigen_rates[:, None] + rates_mine[None, :]
    fine_decay = 1.0 / (1.0 + sums)
    coarse_decay = 1.0 / (1.0 + 2.0 * sums)
    own_part = chain * part
    rates_part = lax.dynamic_slice_in_dim(eigen_rates, own_part, part, 0)
    part_decay = 1.0 / (1.0 + 2.0 * (rates_part[:, None] + rates_mine[None, :]))
    carried_mine = lax.dynamic_slice_in_dim(carried_correction, mine, half, 1)
    carried_part = lax.dynamic_slice_in_dim(carried_mine, own_part, part, 0)

    def swap(x):
        return lax.ppermute(x, "tm", plan.partners())

    def inward(x, shift):
        pieces = [lax.ppermute(x, both, plan.inward(r, shift)) for r in range(plan.rounds)]
        return jnp.concatenate(pieces, 0)

    def outward(x, shift, chains):
        pieces = [
            lax.ppermute(x[r * block : (r + 1) * block], both, plan.outward(r, shift, chains))
            for r in range(plan.rounds)
        ]
        out = pieces[0]
        for r in range(1, plan.rounds):
            out = jnp.where(s % plan.rounds == r, pieces[r], out)
        return out

    def to_eigen(field):
        arrived = swap(dot(field, cols_other))
        kept = dot(field, cols_mine)
        return dot(rows_mine, kept, ((0,), (0,))) + dot(rows_other, arrived, ((0,), (0,)))

    def from_eigen(coeffs):
        arrived = swap(dot(rows_other, coeffs))
        kept = dot(rows_mine, coeffs)
        return dot(kept, cols_mine, ((1,), (1,))) + dot(arrived, cols_other, ((1,), (1,)))

    before = lax.ppermute(guess_coarse[0], "tm", [(g, g + 1) for g in range(groups - 1)])
    before = jnp.where(t == 0, initial_state, before)
    start = inward(reaction(before) + force_fine[0], 0)
    later, start = lax.optimization_barrier(((force_fine[0], force_coarse[0]), start))
    coarse_now = inward(later[1], 0)
    fine_next = inward(later[0], 1)
    coarse_next = inward(later[1], 1)

    relaxed_fine = from_eigen(fine_decay * to_eigen(start))
    coeffs = fine_decay * to_eigen(reaction(relaxed_fine) + coarse_now)
    relaxed_coarse = from_eigen(coeffs)
    second = from_eigen(fine_decay * to_eigen(reaction(relaxed_coarse) + fine_next))
    ahead = fine_decay * to_eigen(reaction(second) + coarse_next)
    term = jnp.where(chain == 0, ahead, ahead - coarse_decay * coeffs)

    rings = plan.rings()
    spread = lax.all_to_all(term, both, 0, 0, axis_index_groups=rings, tiled=True)
    spread = spread.reshape(groups, part, half)
    state = part_decay * carried_part
    states = [state]
    for k in range(groups - 1):
        state = part_decay * state + spread[k]
        states.append(state)
    gathered = jnp.concatenate(states, 0)
    gathered = lax.all_to_all(gathered, both, 0, 0, axis_index_groups=rings, tiled=True)
    total = jnp.where(chain == 0, coarse_decay * carried_mine + coeffs, gathered)

    coarse_new = from_eigen(total)
    fine_new = from_eigen(fine_decay * to_eigen(reaction(coarse_new) + fine_next))
    coarse_out = outward(coarse_new, 0, range(groups))
    first_out = outward(relaxed_fine, 0, range(1))
    fine_out = outward(fine_new, 1, range(groups - 1))
    fine_out = jnp.where(t == 0, first_out, fine_out)
    return (fine_out[None], coarse_out[None])


def solution(mesh):
    placed = (
        P("space", None),
        P("tm", "space", None),
        P("tm", "space", None),
        P("tm", "space", None),
        P(),
        P(),
        P(),
    )
    return jax.shard_map(
        on_device,
        mesh=mesh,
        in_specs=placed,
        out_specs=(P("tm", "space", None), P("tm", "space", None)),
        check_vma=False,
    )
```

```python
import jax
import jax.numpy as jnp
from jax import lax
from jax.experimental import pallas as pl
from jax.sharding import PartitionSpec as P


both = ("tm", "space")


class Plan:
    def __init__(self, groups, blocks):
        self.groups, self.blocks, self.rounds = groups, blocks, blocks // 2
        self.low = blocks // 2 - 1

    def flat(self, t, s):
        return t * self.blocks + s

    def home(self, g, h):
        return self.flat(2 * (g // 2) + h, self.low + g % 2)

    def inward(self, r, shift):
        return [
            (self.flat(g, b), self.home(g - shift, b // self.rounds))
            for g in range(shift, self.groups)
            for b in range(self.blocks)
            if b % self.rounds == r
        ]

    def outward(self, r, shift, chains):
        return [
            (self.home(g, h), self.flat(g + shift, h * self.rounds + r))
            for g in chains
            for h in range(2)
        ]

    def partners(self):
        return [(t, t ^ 1) for t in range(self.groups)]

    def rings(self):
        used = [[self.home(g, h) for g in range(self.groups)] for h in range(2)]
        idle = [s for s in range(self.blocks) if s not in (self.low, self.low + 1)]
        return used + [[self.flat(t, s) for t in range(self.groups)] for s in idle]


def parts(x):
    high = lax.reduce_precision(x, 8, 7)
    return high, lax.reduce_precision(x - high, 8, 7)


def operand(x, axis):
    high, low = parts(x)
    return jnp.concatenate([high, low, high], axis).astype(jnp.bfloat16)


def weight(x, axis):
    high, low = parts(x)
    return jnp.concatenate([high, high, low], axis).astype(jnp.bfloat16)


def dot(left, right):
    return jnp.dot(left, right, preferred_element_type=jnp.float32)


def reaction(field):
    return field + 0.5 * jnp.tanh(field)


def scan_kernel(terms, decay, carried, out):
    state = decay[...] * carried[...]
    out[0] = state
    for k in range(1, out.shape[0]):
        state = decay[...] * state + terms[k - 1]
        out[k] = state


def scan_along(terms, decay, carried):
    chains, rows, columns = terms.shape
    step = min(rows, 32)
    deep = pl.BlockSpec((chains, step, columns), lambda i: (0, i, 0))
    flat = pl.BlockSpec((step, columns), lambda i: (i, 0))
    return pl.pallas_call(
        scan_kernel,
        grid=(rows // step,),
        in_specs=[deep, flat, flat],
        out_specs=deep,
        out_shape=jax.ShapeDtypeStruct(terms.shape, terms.dtype),
        name="scan_along",
    )(terms, decay, carried)


def on_device(
    initial_state,
    guess_coarse,
    force_fine,
    force_coarse,
    eigen_basis,
    eigen_rates,
    carried_correction,
):
    groups, blocks = lax.axis_size("tm"), lax.axis_size("space")
    plan = Plan(groups, blocks)
    t, s = lax.axis_index("tm"), lax.axis_index("space")
    grid = eigen_basis.shape[0]
    half = grid // 2
    part = grid // groups
    block = initial_state.shape[0]
    h = t % 2
    chain = 2 * (t // 2) + jnp.clip(s - plan.low, 0, 1)
    mine, other = h * half, (1 - h) * half

    rows_mine = lax.dynamic_slice_in_dim(eigen_basis, mine, half, 0)
    rows_other = lax.dynamic_slice_in_dim(eigen_basis, other, half, 0)
    cols_mine = lax.dynamic_slice_in_dim(eigen_basis, mine, half, 1)
    cols_other = lax.dynamic_slice_in_dim(eigen_basis, other, half, 1)
    right_mine, right_other = weight(cols_mine, 0), weight(cols_other, 0)
    down_mine, down_other = weight(rows_mine.T, 1), weight(rows_other.T, 1)
    up_mine, up_other = weight(rows_mine, 1), weight(rows_other, 1)
    back_mine, back_other = weight(cols_mine.T, 0), weight(cols_other.T, 0)
    rates_mine = lax.dynamic_slice_in_dim(eigen_rates, mine, half, 0)
    sums = eigen_rates[:, None] + rates_mine[None, :]
    fine_decay = 1.0 / (1.0 + sums)
    coarse_decay = 1.0 / (1.0 + 2.0 * sums)
    own_part = chain * part
    rates_part = lax.dynamic_slice_in_dim(eigen_rates, own_part, part, 0)
    part_decay = 1.0 / (1.0 + 2.0 * (rates_part[:, None] + rates_mine[None, :]))
    carried_mine = lax.dynamic_slice_in_dim(carried_correction, mine, half, 1)
    carried_part = lax.dynamic_slice_in_dim(carried_mine, own_part, part, 0)

    def swap(x):
        return lax.ppermute(x, "tm", plan.partners())

    def inward(pieces, shift):
        out = []
        for r in range(plan.rounds):
            out += [lax.ppermute(x, both, plan.inward(r, shift)) for x in pieces]
        return out

    def outward(pieces, shift, chains):
        pieces = [
            lax.ppermute(x, both, plan.outward(r, shift, chains))
            for r, x in enumerate(pieces)
        ]
        out = pieces[0]
        for r in range(1, plan.rounds):
            out = jnp.where(s % plan.rounds == r, pieces[r], out)
        return out

    def to_eigen(pieces):
        field = operand(jnp.concatenate(pieces, 0), 1)
        arrived = swap(dot(field, right_other))
        kept = dot(down_mine, operand(dot(field, right_mine), 0))
        return kept + dot(down_other, operand(arrived, 0))

    def from_eigen(coeffs):
        coeffs = operand(coeffs, 0)
        arrived = operand(swap(dot(up_other, coeffs)), 1)
        kept = operand(dot(up_mine, coeffs), 1)
        return [
            dot(kept[i : i + block], back_mine) + dot(arrived[i : i + block], back_other)
            for i in range(0, half, block)
        ]

    def forced(fields, forces):
        return [reaction(x) + f for x, f in zip(fields, forces)]

    source_fine, source_coarse = force_fine[0], force_coarse[0]
    cut = block // 2
    started = []
    for c in range(2):
        rows = slice(c * cut, (c + 1) * cut)
        along = [(g, g + 1) for g in range(groups - 1)]
        before = lax.ppermute(guess_coarse[0, rows], "tm", along)
        if started:
            before, started[-1] = lax.optimization_barrier((before, started[-1]))
        before = jnp.where(t == 0, initial_state[rows], before)
        started.append(reaction(before) + source_fine[rows])
    entered = [inward([x], 0) for x in started]
    start = [x for pair in zip(*entered) for x in pair]
    coarse_now = inward([source_coarse], 0)
    fine_next = inward([source_fine], 1)
    coarse_next = inward([source_coarse], 1)

    relaxed_fine = from_eigen(fine_decay * to_eigen(start))
    coeffs = fine_decay * to_eigen(forced(relaxed_fine, coarse_now))
    relaxed_coarse = from_eigen(coeffs)
    second = to_eigen(forced(relaxed_coarse, fine_next))
    second = from_eigen(fine_decay * second)
    ahead = fine_decay * to_eigen(forced(second, coarse_next))
    term = jnp.where(chain == 0, ahead, ahead - coarse_decay * coeffs)

    rings = plan.rings()
    spread = lax.all_to_all(term, both, 0, 0, axis_index_groups=rings, tiled=True)
    states = scan_along(spread.reshape(groups, part, half), part_decay, carried_part)
    states = states.reshape(grid, half)
    states = lax.all_to_all(states, both, 0, 0, axis_index_groups=rings, tiled=True)
    total = jnp.where(chain == 0, coarse_decay * carried_mine + coeffs, states)

    coarse_new = from_eigen(total)
    coarse_out = outward(coarse_new, 0, range(groups))
    fine_new = to_eigen(forced(coarse_new, fine_next))
    fine_new = from_eigen(fine_decay * fine_new)
    fine_out = outward(fine_new, 1, range(groups - 1))
    first_out = outward(relaxed_fine, 0, range(1))
    fine_out = jnp.where(t == 0, first_out, fine_out)
    return (fine_out[None], coarse_out[None])


def solution(mesh):
    placed = (
        P("space", None),
        P("tm", "space", None),
        P("tm", "space", None),
        P("tm", "space", None),
        P(),
        P(),
        P(),
    )
    return jax.shard_map(
        on_device,
        mesh=mesh,
        in_specs=placed,
        out_specs=(P("tm", "space", None), P("tm", "space", None)),
        check_vma=False,
    )
```

```python
import jax
import jax.numpy as jnp
from jax import lax
from jax.experimental import pallas as pl
from jax.sharding import PartitionSpec as P


both = ("tm", "space")


class Plan:
    def __init__(self, groups, blocks):
        self.groups, self.blocks, self.rounds = groups, blocks, blocks // 2
        self.low = blocks // 2 - 1

    def flat(self, t, s):
        return t * self.blocks + s

    def home(self, g, h):
        return self.flat(2 * (g // 2) + h, self.low + g % 2)

    def block(self, h, r):
        return r if h == 0 else self.blocks - 1 - r

    def inward(self, r):
        return [
            (self.flat(g, self.block(h, r)), self.home(g, h))
            for g in range(self.groups)
            for h in range(2)
        ]

    def outward(self, r, shift, chains):
        return [
            (self.home(g, h), self.flat(g + shift, self.block(h, r)))
            for g in chains
            for h in range(2)
        ]

    def partners(self):
        return [(t, t ^ 1) for t in range(self.groups)]

    def rings(self):
        used = [[self.home(g, h) for g in range(self.groups)] for h in range(2)]
        idle = [s for s in range(self.blocks) if s not in (self.low, self.low + 1)]
        return used + [[self.flat(t, s) for t in range(self.groups)] for s in idle]


def parts(x):
    high = lax.reduce_precision(x, 8, 7)
    return high, lax.reduce_precision(x - high, 8, 7)


def operand(x, axis):
    high, low = parts(x)
    return jnp.concatenate([high, low, high], axis).astype(jnp.bfloat16)


def weight(x, axis):
    high, low = parts(x)
    return jnp.concatenate([high, high, low], axis).astype(jnp.bfloat16)


def dot(left, right):
    return jnp.dot(left, right, preferred_element_type=jnp.float32)


def reaction(field):
    return field + 0.5 * jnp.tanh(field)


def scan_kernel(terms, decay, carried, out):
    state = decay[...] * carried[...]
    out[0] = state
    for k in range(1, out.shape[0]):
        state = decay[...] * state + terms[k - 1]
        out[k] = state


def scan_along(terms, decay, carried):
    chains, rows, columns = terms.shape
    step = min(rows, 32)
    deep = pl.BlockSpec((chains, step, columns), lambda i: (0, i, 0))
    flat = pl.BlockSpec((step, columns), lambda i: (i, 0))
    return pl.pallas_call(
        scan_kernel,
        grid=(rows // step,),
        in_specs=[deep, flat, flat],
        out_specs=deep,
        out_shape=jax.ShapeDtypeStruct(terms.shape, terms.dtype),
        name="scan_along",
    )(terms, decay, carried)


def on_device(
    initial_state,
    guess_coarse,
    force_fine,
    force_coarse,
    eigen_basis,
    eigen_rates,
    carried_correction,
):
    groups, blocks = lax.axis_size("tm"), lax.axis_size("space")
    plan = Plan(groups, blocks)
    t, s = lax.axis_index("tm"), lax.axis_index("space")
    grid = eigen_basis.shape[0]
    half = grid // 2
    part = grid // groups
    block = initial_state.shape[0]
    h = t % 2
    chain = 2 * (t // 2) + jnp.clip(s - plan.low, 0, 1)
    mine, other = h * half, (1 - h) * half

    def rows_of(basis, which):
        pieces = []
        for r in range(plan.rounds):
            place = jnp.where(which == 0, plan.block(0, r), plan.block(1, r)) * block
            pieces.append(lax.dynamic_slice_in_dim(basis, place, block, 0))
        return jnp.concatenate(pieces, 0)

    source_fine, source_coarse = force_fine[0], force_coarse[0]
    cut = block // 2
    along = [(g, g + 1) for g in range(groups - 1)]
    shifted = []
    for c in range(2):
        piece = guess_coarse[0, c * cut : (c + 1) * cut]
        shifted.append(lax.ppermute(piece, "tm", along))
    started = []
    for c, before in enumerate(shifted):
        rows = slice(c * cut, (c + 1) * cut)
        if started:
            before, _ = lax.optimization_barrier((before, started[-1]))
        before = jnp.where(t == 0, initial_state[rows], before)
        started.append(reaction(before) + source_fine[rows])
    eigen_basis, _ = lax.optimization_barrier((eigen_basis, started[0]))
    rows_mine = rows_of(eigen_basis, h)
    rows_other = rows_of(eigen_basis, 1 - h)
    cols_mine = lax.dynamic_slice_in_dim(eigen_basis, mine, half, 1)
    cols_other = lax.dynamic_slice_in_dim(eigen_basis, other, half, 1)
    right_mine, right_other = weight(cols_mine, 0), weight(cols_other, 0)
    down_mine, down_other = weight(rows_mine.T, 1), weight(rows_other.T, 1)
    up_mine, up_other = weight(rows_mine, 1), weight(rows_other, 1)
    back_mine, back_other = weight(cols_mine.T, 0), weight(cols_other.T, 0)
    rates_mine = lax.dynamic_slice_in_dim(eigen_rates, mine, half, 0)
    sums = eigen_rates[:, None] + rates_mine[None, :]
    fine_decay = 1.0 / (1.0 + sums)
    coarse_decay = 1.0 / (1.0 + 2.0 * sums)
    own_part = chain * part
    rates_part = lax.dynamic_slice_in_dim(eigen_rates, own_part, part, 0)
    part_decay = 1.0 / (1.0 + 2.0 * (rates_part[:, None] + rates_mine[None, :]))
    carried_mine = lax.dynamic_slice_in_dim(carried_correction, mine, half, 1)
    carried_part = lax.dynamic_slice_in_dim(carried_mine, own_part, part, 0)

    def swap(x):
        return lax.ppermute(x, "tm", plan.partners())

    def inward(x, r):
        return lax.ppermute(x, both, plan.inward(r))

    def outward(pieces, shift, chains):
        pieces = [
            lax.ppermute(x, both, plan.outward(r, shift, chains))
            for r, x in enumerate(pieces)
        ]
        out = pieces[0]
        for r in range(1, plan.rounds):
            out = jnp.where(jnp.minimum(s, blocks - 1 - s) == r, pieces[r], out)
        return out

    def to_eigen(pieces):
        field = operand(jnp.concatenate(pieces, 0), 1)
        arrived = swap(dot(field, right_other))
        kept = dot(down_mine, operand(dot(field, right_mine), 0))
        return kept + dot(down_other, operand(arrived, 0))

    def from_eigen(coeffs):
        coeffs = operand(coeffs, 0)
        arrived = operand(swap(dot(up_other, coeffs)), 1)
        kept = operand(dot(up_mine, coeffs), 1)
        return [
            dot(kept[i : i + block], back_mine) + dot(arrived[i : i + block], back_other)
            for i in range(0, half, block)
        ]

    def forced(fields, forces):
        return [reaction(x) + f for x, f in zip(fields, forces)]

    later_fine = lax.ppermute(source_fine, "tm", [(g + 1, g) for g in range(groups - 1)])
    later_coarse = lax.ppermute(
        source_coarse, "tm", [(g + 1, g) for g in range(groups - 1)]
    )
    rounds = range(plan.rounds)
    start = [inward(x, r) for r in rounds for x in started]
    coarse_now = [inward(source_coarse, r) for r in rounds]
    fine_next = [inward(later_fine, r) for r in rounds]
    coarse_next = [inward(later_coarse, r) for r in rounds]

    relaxed_fine = from_eigen(fine_decay * to_eigen(start))
    coeffs = fine_decay * to_eigen(forced(relaxed_fine, coarse_now))
    relaxed_coarse = from_eigen(coeffs)
    second = to_eigen(forced(relaxed_coarse, fine_next))
    second = from_eigen(fine_decay * second)
    ahead = fine_decay * to_eigen(forced(second, coarse_next))
    term = jnp.where(chain == 0, ahead, ahead - coarse_decay * coeffs)

    rings = plan.rings()
    spread = lax.all_to_all(term, both, 0, 0, axis_index_groups=rings, tiled=True)
    states = scan_along(spread.reshape(groups, part, half), part_decay, carried_part)
    states = states.reshape(grid, half)
    states = lax.all_to_all(states, both, 0, 0, axis_index_groups=rings, tiled=True)
    total = jnp.where(chain == 0, coarse_decay * carried_mine + coeffs, states)

    coarse_new = from_eigen(total)
    coarse_out = outward(coarse_new, 0, range(groups))
    fine_new = to_eigen(forced(coarse_new, fine_next))
    fine_new = from_eigen(fine_decay * fine_new)
    fine_out = outward(fine_new, 1, range(groups - 1))
    first_out = outward(relaxed_fine, 0, range(1))
    fine_out = jnp.where(t == 0, first_out, fine_out)
    return (fine_out[None], coarse_out[None])


def solution(mesh):
    placed = (
        P("space", None),
        P("tm", "space", None),
        P("tm", "space", None),
        P("tm", "space", None),
        P(),
        P(),
        P(),
    )
    return jax.shard_map(
        on_device,
        mesh=mesh,
        in_specs=placed,
        out_specs=(P("tm", "space", None), P("tm", "space", None)),
        check_vma=False,
    )
```

```python
import jax
import jax.numpy as jnp
from jax import lax
from jax.experimental import pallas as pl
from jax.sharding import PartitionSpec as P


both = ("tm", "space")


class Plan:
    def __init__(self, groups, blocks):
        self.groups, self.blocks, self.rounds = groups, blocks, blocks // 2
        self.low = blocks // 2 - 1

    def flat(self, t, s):
        return t * self.blocks + s

    def home(self, g, h):
        return self.flat(2 * (g // 2) + h, self.low + g % 2)

    def block(self, h, r):
        return r if h == 0 else self.blocks - 1 - r

    def inward(self, r):
        return [
            (self.flat(g, self.block(h, r)), self.home(g, h))
            for g in range(self.groups)
            for h in range(2)
        ]

    def outward(self, r, shift, chains):
        return [
            (self.home(g, h), self.flat(g + shift, self.block(h, r)))
            for g in chains
            for h in range(2)
        ]

    def partners(self):
        return [(t, t ^ 1) for t in range(self.groups)]

    def rings(self):
        used = [[self.home(g, h) for g in range(self.groups)] for h in range(2)]
        idle = [s for s in range(self.blocks) if s not in (self.low, self.low + 1)]
        return used + [[self.flat(t, s) for t in range(self.groups)] for s in idle]


def parts(x):
    high = lax.reduce_precision(x, 8, 7)
    return high, lax.reduce_precision(x - high, 8, 7)


def operand(x, axis):
    high, low = parts(x)
    return jnp.concatenate([high, low, high], axis).astype(jnp.bfloat16)


def weight(x, axis):
    high, low = parts(x)
    return jnp.concatenate([high, high, low], axis).astype(jnp.bfloat16)


def dot(left, right):
    return jnp.dot(left, right, preferred_element_type=jnp.float32)


def reaction(field):
    return field + 0.5 * jnp.tanh(field)


def scan_kernel(terms, decay, carried, out):
    state = decay[...] * carried[...]
    out[0] = state
    for k in range(1, out.shape[0]):
        state = decay[...] * state + terms[k - 1]
        out[k] = state


def scan_along(terms, decay, carried):
    chains, rows, columns = terms.shape
    step = min(rows, 32)
    deep = pl.BlockSpec((chains, step, columns), lambda i: (0, i, 0))
    flat = pl.BlockSpec((step, columns), lambda i: (i, 0))
    return pl.pallas_call(
        scan_kernel,
        grid=(rows // step,),
        in_specs=[deep, flat, flat],
        out_specs=deep,
        out_shape=jax.ShapeDtypeStruct(terms.shape, terms.dtype),
        name="scan_along",
    )(terms, decay, carried)


def on_device(
    initial_state,
    guess_coarse,
    force_fine,
    force_coarse,
    eigen_basis,
    eigen_rates,
    carried_correction,
):
    groups, blocks = lax.axis_size("tm"), lax.axis_size("space")
    plan = Plan(groups, blocks)
    t, s = lax.axis_index("tm"), lax.axis_index("space")
    grid = eigen_basis.shape[0]
    half = grid // 2
    part = grid // groups
    block = initial_state.shape[0]
    h = t % 2
    chain = 2 * (t // 2) + jnp.clip(s - plan.low, 0, 1)
    mine, other = h * half, (1 - h) * half

    def rows_of(basis, which):
        pieces = []
        for r in range(plan.rounds):
            place = jnp.where(which == 0, plan.block(0, r), plan.block(1, r)) * block
            pieces.append(lax.dynamic_slice_in_dim(basis, place, block, 0))
        return jnp.concatenate(pieces, 0)

    source_fine, source_coarse = force_fine[0], force_coarse[0]
    cut = block // 2
    along = [(g, g + 1) for g in range(groups - 1)]
    shifted = []
    for c in range(2):
        piece = guess_coarse[0, c * cut : (c + 1) * cut]
        shifted.append(lax.ppermute(piece, "tm", along))
    started = []
    for c, before in enumerate(shifted):
        rows = slice(c * cut, (c + 1) * cut)
        if started:
            before, _ = lax.optimization_barrier((before, started[-1]))
        before = jnp.where(t == 0, initial_state[rows], before)
        started.append(reaction(before) + source_fine[rows])
    eigen_basis, _ = lax.optimization_barrier((eigen_basis, started[0]))
    rows_mine = rows_of(eigen_basis, h)
    rows_other = rows_of(eigen_basis, 1 - h)
    cols_mine = lax.dynamic_slice_in_dim(eigen_basis, mine, half, 1)
    cols_other = lax.dynamic_slice_in_dim(eigen_basis, other, half, 1)
    right_mine, right_other = weight(cols_mine, 0), weight(cols_other, 0)
    down_mine, down_other = weight(rows_mine.T, 1), weight(rows_other.T, 1)
    up_mine, up_other = weight(rows_mine, 1), weight(rows_other, 1)
    back_mine, back_other = weight(cols_mine.T, 0), weight(cols_other.T, 0)
    rates_mine = lax.dynamic_slice_in_dim(eigen_rates, mine, half, 0)
    sums = eigen_rates[:, None] + rates_mine[None, :]
    fine_decay = 1.0 / (1.0 + sums)
    coarse_decay = 1.0 / (1.0 + 2.0 * sums)
    own_part = chain * part
    rates_part = lax.dynamic_slice_in_dim(eigen_rates, own_part, part, 0)
    part_decay = 1.0 / (1.0 + 2.0 * (rates_part[:, None] + rates_mine[None, :]))
    carried_part = lax.dynamic_slice(carried_correction, (own_part, mine), (part, half))

    def swap(x):
        return lax.ppermute(x, "tm", plan.partners())

    def sent(x, pairs):
        return lax.ppermute(x, both, [(a, b) for a, b in pairs if a != b])

    def with_kept(x, out, pairs):
        stays = False
        for a, b in pairs:
            if a == b:
                stays = stays | (t * blocks + s == a)
        return out if stays is False else jnp.where(stays, x, out)

    def inward(x, r):
        return with_kept(x, sent(x, plan.inward(r)), plan.inward(r))

    def outward(pieces, shift, chains):
        out = []
        for r, x in enumerate(pieces):
            out.append(sent(x, plan.outward(r, shift, chains)))
        return out

    def settled(pieces, arrived, shift, chains):
        out = None
        for r, x in enumerate(pieces):
            here = with_kept(x, arrived[r], plan.outward(r, shift, chains))
            out = here if r == 0 else jnp.where(jnp.minimum(s, blocks - 1 - s) == r, here, out)
        return out

    def to_eigen(pieces):
        field = operand(jnp.concatenate(pieces, 0), 1)
        arrived = swap(dot(field, right_other))
        kept = dot(down_mine, operand(dot(field, right_mine), 0))
        return kept + dot(down_other, operand(arrived, 0))

    def from_eigen(coeffs):
        coeffs = operand(coeffs, 0)
        arrived = operand(swap(dot(up_other, coeffs)), 1)
        kept = operand(dot(up_mine, coeffs), 1)
        out = []
        for r in range(plan.rounds):
            rows = slice(r * block, (r + 1) * block)
            early = dot(kept[rows], back_mine)
            out.append(early + dot(arrived[rows], back_other))
        return out

    def forced(fields, forces):
        return [reaction(x) + f for x, f in zip(fields, forces)]

    later_fine = lax.ppermute(source_fine, "tm", [(g + 1, g) for g in range(groups - 1)])
    later_coarse = lax.ppermute(
        source_coarse, "tm", [(g + 1, g) for g in range(groups - 1)]
    )
    rounds = range(plan.rounds)
    start = [inward(x, r) for r in rounds for x in started]
    coarse_now = [inward(source_coarse, r) for r in rounds]
    fine_next = [inward(later_fine, r) for r in rounds]
    coarse_next = [inward(later_coarse, r) for r in rounds]

    relaxed_fine = from_eigen(fine_decay * to_eigen(start))
    coeffs = fine_decay * to_eigen(forced(relaxed_fine, coarse_now))
    relaxed_coarse = from_eigen(coeffs)
    first = chain == 0
    second = to_eigen(forced(relaxed_coarse, fine_next))
    second = from_eigen(fine_decay * second)
    ahead = fine_decay * to_eigen(forced(second, coarse_next))
    term = jnp.where(first, ahead, ahead - coarse_decay * coeffs)

    rings = plan.rings()
    spread = lax.all_to_all(term, both, 0, 0, axis_index_groups=rings, tiled=True)
    states = scan_along(spread.reshape(groups, part, half), part_decay, carried_part)
    states = states.reshape(grid, half)
    states = lax.all_to_all(states, both, 0, 0, axis_index_groups=rings, tiled=True)
    total = states + jnp.where(first, coeffs, 0.0)

    coarse_new = from_eigen(total)
    coarse_sent = outward(coarse_new, 0, range(groups))
    fine_new = to_eigen(forced(coarse_new, fine_next))
    fine_new = from_eigen(fine_decay * fine_new)
    fine_sent = outward(fine_new, 1, range(groups - 1))
    first_sent = outward(relaxed_fine, 0, range(1))
    coarse_new, relaxed_fine, fine_new = lax.optimization_barrier(
        (coarse_new, relaxed_fine, fine_new)
    )
    first_out = settled(relaxed_fine, first_sent, 0, range(1))
    coarse_out = settled(coarse_new, coarse_sent, 0, range(groups))
    coarse_out, first_out = lax.optimization_barrier((coarse_out, first_out))
    fine_out = settled(fine_new, fine_sent, 1, range(groups - 1))
    fine_out = jnp.where(t == 0, first_out, fine_out)
    return (fine_out[None], coarse_out[None])


def solution(mesh):
    placed = (
        P("space", None),
        P("tm", "space", None),
        P("tm", "space", None),
        P("tm", "space", None),
        P(),
        P(),
        P(),
    )
    return jax.shard_map(
        on_device,
        mesh=mesh,
        in_specs=placed,
        out_specs=(P("tm", "space", None), P("tm", "space", None)),
        check_vma=False,
    )
```

```python
import jax
import jax.numpy as jnp
from jax import lax
from jax.experimental import pallas as pl
from jax.experimental.pallas import tpu as pltpu
from jax.sharding import PartitionSpec as P


both = ("tm", "space")


class Plan:
    def __init__(self, groups, blocks):
        self.groups, self.blocks, self.rounds = groups, blocks, blocks // 2
        self.low = blocks // 2 - 1

    def flat(self, t, s):
        return t * self.blocks + s

    def home(self, g, h):
        return self.flat(2 * (g // 2) + h, self.low + g % 2)

    def block(self, h, r):
        return r if h == 0 else self.blocks - 1 - r

    def inward(self, r):
        return [
            (self.flat(g, self.block(h, r)), self.home(g, h))
            for g in range(self.groups)
            for h in range(2)
        ]

    def outward(self, r, shift, chains):
        return [
            (self.home(g, h), self.flat(g + shift, self.block(h, r)))
            for g in chains
            for h in range(2)
        ]

    def partners(self):
        return [(t, t ^ 1) for t in range(self.groups)]

    def rings(self):
        used = [[self.home(g, h) for g in range(self.groups)] for h in range(2)]
        idle = [s for s in range(self.blocks) if s not in (self.low, self.low + 1)]
        return used + [[self.flat(t, s) for t in range(self.groups)] for s in idle]


def parts(x):
    high = lax.reduce_precision(x, 8, 7)
    return high, lax.reduce_precision(x - high, 8, 7)


def operand(x, axis):
    high, low = parts(x)
    return jnp.concatenate([high, low, high], axis).astype(jnp.bfloat16)


def weight(x, axis):
    high, low = parts(x)
    return jnp.concatenate([high, high, low], axis).astype(jnp.bfloat16)


def dot(left, right):
    return jnp.dot(left, right, preferred_element_type=jnp.float32)


def reaction(field):
    return field + 0.5 * jnp.tanh(field)


def scan_kernel(terms, decay, carried, out):
    count, rows, _ = out.shape
    step = min(rows, 16)

    def body(i, _):
        at = pl.ds(i * step, step)
        factor = decay[at]
        state = factor * carried[at]
        out[0, at] = state
        for k in range(1, count):
            state = factor * state + terms[k - 1, at]
            out[k, at] = state
        return 0

    lax.fori_loop(0, rows // step, body, 0)


def scan_along(terms, decay, carried):
    whole = pl.BlockSpec(memory_space=pltpu.VMEM)
    return pl.pallas_call(
        scan_kernel,
        in_specs=[whole] * 3,
        out_specs=whole,
        out_shape=jax.ShapeDtypeStruct(terms.shape, terms.dtype),
        compiler_params=pltpu.CompilerParams(vmem_limit_bytes=4 * terms.size * 2 + (4 << 20)),
        name="scan_along",
    )(terms, decay, carried)


def on_device(
    initial_state,
    guess_coarse,
    force_fine,
    force_coarse,
    eigen_basis,
    eigen_rates,
    carried_correction,
):
    groups, blocks = lax.axis_size("tm"), lax.axis_size("space")
    plan = Plan(groups, blocks)
    t, s = lax.axis_index("tm"), lax.axis_index("space")
    grid = eigen_basis.shape[0]
    half = grid // 2
    part = grid // groups
    block = initial_state.shape[0]
    h = t % 2
    chain = 2 * (t // 2) + jnp.clip(s - plan.low, 0, 1)
    mine, other = h * half, (1 - h) * half

    def rows_of(basis, which):
        pieces = []
        for r in range(plan.rounds):
            place = jnp.where(which == 0, plan.block(0, r), plan.block(1, r)) * block
            pieces.append(lax.dynamic_slice_in_dim(basis, place, block, 0))
        return jnp.concatenate(pieces, 0)

    source_fine, source_coarse = force_fine[0], force_coarse[0]
    cut = block // 2
    along = [(g, g + 1) for g in range(groups - 1)]
    shifted = []
    for c in range(2):
        piece = guess_coarse[0, c * cut : (c + 1) * cut]
        shifted.append(lax.ppermute(piece, "tm", along))
    started = []
    for c, before in enumerate(shifted):
        rows = slice(c * cut, (c + 1) * cut)
        if started:
            before, _ = lax.optimization_barrier((before, started[-1]))
        before = jnp.where(t == 0, initial_state[rows], before)
        started.append(reaction(before) + source_fine[rows])
    eigen_basis, eigen_rates, carried_correction, _ = lax.optimization_barrier(
        (eigen_basis, eigen_rates, carried_correction, started[0])
    )
    rows_mine = rows_of(eigen_basis, h)
    rows_other = rows_of(eigen_basis, 1 - h)
    cols_mine = lax.dynamic_slice_in_dim(eigen_basis, mine, half, 1)
    cols_other = lax.dynamic_slice_in_dim(eigen_basis, other, half, 1)
    right_mine, right_other = weight(cols_mine, 0), weight(cols_other, 0)
    down_mine, down_other = weight(rows_mine.T, 1), weight(rows_other.T, 1)
    up_mine, up_other = weight(rows_mine, 1), weight(rows_other, 1)
    back_mine, back_other = weight(cols_mine.T, 0), weight(cols_other.T, 0)
    rates_mine = lax.dynamic_slice_in_dim(eigen_rates, mine, half, 0)
    sums = eigen_rates[:, None] + rates_mine[None, :]
    fine_decay = 1.0 / (1.0 + sums)
    coarse_decay = 1.0 / (1.0 + 2.0 * sums)
    own_part = chain * part
    rates_part = lax.dynamic_slice_in_dim(eigen_rates, own_part, part, 0)
    part_decay = 1.0 / (1.0 + 2.0 * (rates_part[:, None] + rates_mine[None, :]))
    carried_part = lax.dynamic_slice(carried_correction, (own_part, mine), (part, half))

    def swap(x):
        return lax.ppermute(x, "tm", plan.partners())

    def sent(x, pairs):
        return lax.ppermute(x, both, [(a, b) for a, b in pairs if a != b])

    def with_kept(x, out, pairs):
        stays = False
        for a, b in pairs:
            if a == b:
                stays = stays | (t * blocks + s == a)
        return out if stays is False else jnp.where(stays, x, out)

    def inward(x, r):
        return with_kept(x, sent(x, plan.inward(r)), plan.inward(r))

    def outward(pieces, shift, chains):
        out = []
        for r, x in enumerate(pieces):
            out.append(sent(x, plan.outward(r, shift, chains)))
        return out

    def settled(pieces, arrived, shift, chains):
        out = None
        for r, x in enumerate(pieces):
            here = with_kept(x, arrived[r], plan.outward(r, shift, chains))
            out = here if r == 0 else jnp.where(jnp.minimum(s, blocks - 1 - s) == r, here, out)
        return out

    def to_eigen(pieces):
        field = operand(jnp.concatenate(pieces, 0), 1)
        arrived = swap(dot(field, right_other))
        kept = dot(down_mine, operand(dot(field, right_mine), 0))
        return kept + dot(down_other, operand(arrived, 0))

    def from_eigen(coeffs):
        coeffs = operand(coeffs, 0)
        arrived = operand(swap(dot(up_other, coeffs)), 1)
        kept = operand(dot(up_mine, coeffs), 1)
        out = []
        for r in range(plan.rounds):
            rows = slice(r * block, (r + 1) * block)
            early = dot(kept[rows], back_mine)
            out.append(early + dot(arrived[rows], back_other))
        return out

    def forced(fields, forces):
        return [reaction(x) + f for x, f in zip(fields, forces)]

    later_fine = lax.ppermute(source_fine, "tm", [(g + 1, g) for g in range(groups - 1)])
    later_coarse = lax.ppermute(
        source_coarse, "tm", [(g + 1, g) for g in range(groups - 1)]
    )
    rounds = range(plan.rounds)
    start = [inward(x, r) for r in rounds for x in started]
    coarse_now = [inward(source_coarse, r) for r in rounds]
    fine_next = [inward(later_fine, r) for r in rounds]
    coarse_next = [inward(later_coarse, r) for r in rounds]

    relaxed_fine = from_eigen(fine_decay * to_eigen(start))
    coeffs = fine_decay * to_eigen(forced(relaxed_fine, coarse_now))
    relaxed_coarse = from_eigen(coeffs)
    first = chain == 0
    second = to_eigen(forced(relaxed_coarse, fine_next))
    second = from_eigen(fine_decay * second)
    ahead = fine_decay * to_eigen(forced(second, coarse_next))
    term = jnp.where(first, ahead, ahead - coarse_decay * coeffs)

    rings = plan.rings()
    spread = lax.all_to_all(term, both, 0, 0, axis_index_groups=rings, tiled=True)
    states = scan_along(spread.reshape(groups, part, half), part_decay, carried_part)
    states = states.reshape(grid, half)
    states = lax.all_to_all(states, both, 0, 0, axis_index_groups=rings, tiled=True)
    total = states + jnp.where(first, coeffs, 0.0)

    coarse_new = from_eigen(total)
    coarse_sent = outward(coarse_new, 0, range(groups))
    fine_new = to_eigen(forced(coarse_new, fine_next))
    fine_new = from_eigen(fine_decay * fine_new)
    fine_sent = outward(fine_new, 1, range(groups - 1))
    first_sent = outward(relaxed_fine, 0, range(1))
    coarse_new, relaxed_fine, fine_new = lax.optimization_barrier(
        (coarse_new, relaxed_fine, fine_new)
    )
    first_out = settled(relaxed_fine, first_sent, 0, range(1))
    coarse_out = settled(coarse_new, coarse_sent, 0, range(groups))
    coarse_out, first_out = lax.optimization_barrier((coarse_out, first_out))
    fine_out = settled(fine_new, fine_sent, 1, range(groups - 1))
    fine_out = jnp.where(t == 0, first_out, fine_out)
    return (fine_out[None], coarse_out[None])


def solution(mesh):
    placed = (
        P("space", None),
        P("tm", "space", None),
        P("tm", "space", None),
        P("tm", "space", None),
        P(),
        P(),
        P(),
    )
    return jax.shard_map(
        on_device,
        mesh=mesh,
        in_specs=placed,
        out_specs=(P("tm", "space", None), P("tm", "space", None)),
        check_vma=False,
    )
```

```python
import jax
import jax.numpy as jnp
from jax import lax
from jax.experimental import pallas as pl
from jax.experimental.pallas import tpu as pltpu
from jax.sharding import PartitionSpec as P


both = ("tm", "space")


class Plan:
    def __init__(self, groups, blocks):
        self.groups, self.blocks, self.rounds = groups, blocks, blocks // 2
        self.low = blocks // 2 - 1

    def flat(self, t, s):
        return t * self.blocks + s

    def home(self, g, h):
        return self.flat(2 * (g // 2) + h, self.low + g % 2)

    def block(self, h, r):
        return r if h == 0 else self.blocks - 1 - r

    def inward(self, r):
        return [
            (self.flat(g, self.block(h, r)), self.home(g, h))
            for g in range(self.groups)
            for h in range(2)
        ]

    def outward(self, r, shift, chains):
        return [
            (self.home(g, h), self.flat(g + shift, self.block(h, r)))
            for g in chains
            for h in range(2)
        ]

    def partners(self):
        return [(t, t ^ 1) for t in range(self.groups)]

    def rings(self):
        used = [[self.home(g, h) for g in range(self.groups)] for h in range(2)]
        idle = [s for s in range(self.blocks) if s not in (self.low, self.low + 1)]
        return used + [[self.flat(t, s) for t in range(self.groups)] for s in idle]


def parts(x):
    high = lax.reduce_precision(x, 8, 7)
    return high, lax.reduce_precision(x - high, 8, 7)


def operand(x, axis):
    high, low = parts(x)
    return jnp.concatenate([high, low, high], axis).astype(jnp.bfloat16)


def weight(x, axis):
    high, low = parts(x)
    return jnp.concatenate([high, high, low], axis).astype(jnp.bfloat16)


def dot(left, right):
    return jnp.dot(left, right, preferred_element_type=jnp.float32)


def reaction(field):
    return field + 0.5 * jnp.tanh(field)


def scan_kernel(terms, decay, carried, out):
    count, rows, _ = out.shape
    step = min(rows, 16)

    def body(i, _):
        at = pl.ds(i * step, step)
        factor = decay[at]
        state = factor * carried[at]
        out[0, at] = state
        for k in range(1, count):
            state = factor * state + terms[k - 1, at]
            out[k, at] = state
        return 0

    lax.fori_loop(0, rows // step, body, 0)


def scan_along(terms, decay, carried):
    whole = pl.BlockSpec(memory_space=pltpu.VMEM)
    return pl.pallas_call(
        scan_kernel,
        in_specs=[whole] * 3,
        out_specs=whole,
        out_shape=jax.ShapeDtypeStruct(terms.shape, terms.dtype),
        compiler_params=pltpu.CompilerParams(vmem_limit_bytes=4 * terms.size * 2 + (4 << 20)),
        name="scan_along",
    )(terms, decay, carried)


def on_device(
    initial_state,
    guess_coarse,
    force_fine,
    force_coarse,
    eigen_basis,
    eigen_rates,
    carried_correction,
):
    groups, blocks = lax.axis_size("tm"), lax.axis_size("space")
    plan = Plan(groups, blocks)
    t, s = lax.axis_index("tm"), lax.axis_index("space")
    grid = eigen_basis.shape[0]
    half = grid // 2
    part = grid // groups
    block = initial_state.shape[0]
    h = t % 2
    chain = 2 * (t // 2) + jnp.clip(s - plan.low, 0, 1)
    mine, other = h * half, (1 - h) * half

    def rows_of(basis, which):
        pieces = []
        for r in range(plan.rounds):
            place = jnp.where(which == 0, plan.block(0, r), plan.block(1, r)) * block
            pieces.append(lax.dynamic_slice_in_dim(basis, place, block, 0))
        return jnp.concatenate(pieces, 0)

    source_fine, source_coarse = force_fine[0], force_coarse[0]
    cut = block // 2
    along = [(g, g + 1) for g in range(groups - 1)]
    shifted = []
    for c in range(2):
        piece = guess_coarse[0, c * cut : (c + 1) * cut]
        shifted.append(lax.ppermute(piece, "tm", along))
    started = []
    for c, before in enumerate(shifted):
        rows = slice(c * cut, (c + 1) * cut)
        if started:
            before, _ = lax.optimization_barrier((before, started[-1]))
        before = jnp.where(t == 0, initial_state[rows], before)
        started.append(reaction(before) + source_fine[rows])
    eigen_basis, eigen_rates, carried_correction, _ = lax.optimization_barrier(
        (eigen_basis, eigen_rates, carried_correction, started[0])
    )
    rows_mine = rows_of(eigen_basis, h)
    rows_other = rows_of(eigen_basis, 1 - h)
    cols_mine = lax.dynamic_slice_in_dim(eigen_basis, mine, half, 1)
    cols_other = lax.dynamic_slice_in_dim(eigen_basis, other, half, 1)
    right_mine, right_other = weight(cols_mine, 0), weight(cols_other, 0)
    down_mine, down_other = weight(rows_mine.T, 1), weight(rows_other.T, 1)
    up_mine, up_other = weight(rows_mine, 1), weight(rows_other, 1)
    back_mine, back_other = weight(cols_mine.T, 0), weight(cols_other.T, 0)
    rates_mine = lax.dynamic_slice_in_dim(eigen_rates, mine, half, 0)
    sums = eigen_rates[:, None] + rates_mine[None, :]
    fine_decay = 1.0 / (1.0 + sums)
    coarse_decay = 1.0 / (1.0 + 2.0 * sums)
    own_part = chain * part
    rates_part = lax.dynamic_slice_in_dim(eigen_rates, own_part, part, 0)
    part_decay = 1.0 / (1.0 + 2.0 * (rates_part[:, None] + rates_mine[None, :]))
    carried_part = lax.dynamic_slice(carried_correction, (own_part, mine), (part, half))

    def swap(x):
        return lax.ppermute(x, "tm", plan.partners())

    def sent(x, pairs):
        return lax.ppermute(x, both, [(a, b) for a, b in pairs if a != b])

    def with_kept(x, out, pairs):
        stays = False
        for a, b in pairs:
            if a == b:
                stays = stays | (t * blocks + s == a)
        return out if stays is False else jnp.where(stays, x, out)

    def inward(x, r):
        return with_kept(x, sent(x, plan.inward(r)), plan.inward(r))

    def outward(pieces, shift, chains):
        out = []
        for r, x in enumerate(pieces):
            out.append(sent(x, plan.outward(r, shift, chains)))
        return out

    def settled(pieces, arrived, shift, chains):
        out = None
        for r, x in enumerate(pieces):
            here = with_kept(x, arrived[r], plan.outward(r, shift, chains))
            out = here if r == 0 else jnp.where(jnp.minimum(s, blocks - 1 - s) == r, here, out)
        return out

    def to_eigen(pieces):
        field = operand(jnp.concatenate(pieces, 0), 1)
        arrived = swap(dot(field, right_other))
        kept = dot(down_mine, operand(dot(field, right_mine), 0))
        return kept + dot(down_other, operand(arrived, 0))

    def from_eigen(coeffs, whole=False):
        coeffs = operand(coeffs, 0)
        arrived = operand(swap(dot(up_other, coeffs)), 1)
        kept = operand(dot(up_mine, coeffs), 1)
        if whole:
            return [dot(kept, back_mine) + dot(arrived, back_other)]
        out = []
        for r in range(plan.rounds):
            rows = slice(r * block, (r + 1) * block)
            early = dot(kept[rows], back_mine)
            out.append(early + dot(arrived[rows], back_other))
        return out

    def forced(fields, forces):
        return [reaction(x) + f for x, f in zip(fields, forces)]

    later_fine = lax.ppermute(source_fine, "tm", [(g + 1, g) for g in range(groups - 1)])
    later_coarse = lax.ppermute(
        source_coarse, "tm", [(g + 1, g) for g in range(groups - 1)]
    )
    rounds = range(plan.rounds)
    start = [inward(x, r) for r in rounds for x in started]
    coarse_now = [inward(source_coarse, r) for r in rounds]
    fine_next = [inward(later_fine, r) for r in rounds]
    coarse_next = [inward(later_coarse, r) for r in rounds]

    relaxed_fine = from_eigen(fine_decay * to_eigen(start))
    coeffs = fine_decay * to_eigen(forced(relaxed_fine, coarse_now))
    relaxed_coarse = from_eigen(coeffs, True)
    first = chain == 0
    second = to_eigen(forced(relaxed_coarse, [jnp.concatenate(fine_next, 0)]))
    second = from_eigen(fine_decay * second, True)
    ahead = fine_decay * to_eigen(forced(second, [jnp.concatenate(coarse_next, 0)]))
    term = jnp.where(first, ahead, ahead - coarse_decay * coeffs)

    rings = plan.rings()
    spread = lax.all_to_all(term, both, 0, 0, axis_index_groups=rings, tiled=True)
    states = scan_along(spread.reshape(groups, part, half), part_decay, carried_part)
    states = states.reshape(grid, half)
    states = lax.all_to_all(states, both, 0, 0, axis_index_groups=rings, tiled=True)
    total = states + jnp.where(first, coeffs, 0.0)

    coarse_new = from_eigen(total)
    coarse_sent = outward(coarse_new, 0, range(groups))
    fine_new = to_eigen(forced(coarse_new, fine_next))
    fine_new = from_eigen(fine_decay * fine_new)
    fine_sent = outward(fine_new, 1, range(groups - 1))
    first_sent = outward(relaxed_fine, 0, range(1))
    coarse_new, relaxed_fine, fine_new = lax.optimization_barrier(
        (coarse_new, relaxed_fine, fine_new)
    )
    first_out = settled(relaxed_fine, first_sent, 0, range(1))
    coarse_out = settled(coarse_new, coarse_sent, 0, range(groups))
    coarse_out, first_out = lax.optimization_barrier((coarse_out, first_out))
    fine_out = settled(fine_new, fine_sent, 1, range(groups - 1))
    fine_out = jnp.where(t == 0, first_out, fine_out)
    return (fine_out[None], coarse_out[None])


def solution(mesh):
    placed = (
        P("space", None),
        P("tm", "space", None),
        P("tm", "space", None),
        P("tm", "space", None),
        P(),
        P(),
        P(),
    )
    return jax.shard_map(
        on_device,
        mesh=mesh,
        in_specs=placed,
        out_specs=(P("tm", "space", None), P("tm", "space", None)),
        check_vma=False,
    )
```
